32 devices in a mesh: grp: 2 (over x), exp: 16 (over z, y, core).
Axes of the slice: x: 2, y: 2, z: 4, core: 2. Of those that a mesh axis runs over, the one named last changes fastest.
Arguments:
- tokens: bfloat16 [192, 196, 768], P(('grp', 'exp')), parts along dimension 0, may hold values from -6 to 6
- logits: float32 [192, 196, 16], P(('grp', 'exp')), parts along dimension 0, may hold values from -8 to 400
- slot_out: bfloat16 [32, 96, 768], P(('grp', 'exp')), parts along dimension 0, may hold values from -1.5 to 1.5
- slot_in: bfloat16 [32, 96, 768], P(('grp', 'exp')), parts along dimension 0, may hold values from -6 to 6
- out_grad: bfloat16 [192, 196, 768], P(('grp', 'exp')), parts along dimension 0, may hold values from -192 to 192
- router: bfloat16 [16, 768], replicated, may hold values from -0.21875 to 0.21875
- w_in: bfloat16 [16, 768, 3072], P('exp'), may hold values from -0.21875 to 0.21875
- bias_in: float32 [16, 3072], P('exp'), may hold values from -5 to 5
- w_out: bfloat16 [16, 3072, 768], P('exp'), may hold values from -0.109375 to 0.109375
Outputs:
- input_grad: bfloat16 [192, 196, 768], P(('grp', 'exp')), parts along dimension 0
- router_grad: float32 [32, 768], P(('grp', 'exp')), parts along dimension 0
The draws below stay inside these ranges and needn't reach their ends.
There are 2 independent parts, one for each index of `grp`. The reference program is written for one: setup_inputs(seed, part) draws one part's arguments, and reference() takes and returns one part's arrays. A program takes and returns all parts, laid end to end along the dimension named above; an argument that names none is the same for every part. Nothing has to cross between parts.
All inputs are finite; a program needn't handle non-finite values.
Results may differ from the reference program's by a relative error of at most 0.0075.
Values may be sent and summed in bfloat16 or wider, within the bound.
A program may use at most 64 MiB of HBM per device.

```python
import jax
import jax.numpy as jnp
from jax import lax

D = 768
FF = 3072
SEQ = 196
EXPERTS = 16
IMAGES = 96


def draw_logits(key, part):
    base = jnp.clip(1.5 * jax.random.normal(key, (IMAGES, SEQ, EXPERTS), jnp.float32), -6.0, 6.0)
    return base


def steps_of(stream_key, dims, shards, least, high):
    def one(axis_at, parts):
        steps = jax.random.uniform(jax.random.fold_in(jax.random.fold_in(stream_key, 6), axis_at), (parts,), jnp.float32, least / len(shards), high / len(shards))
        return jnp.repeat(jnp.exp(steps), dims[axis_at] // parts).reshape((-1,) + (1,) * (len(dims) - axis_at - 1))

    loudness = one(*shards[0])
    for cut in shards[1:]:
        loudness = loudness * one(*cut)
    return loudness


def noise(stream_key, extent, width, most, shards=(), dtype=jnp.bfloat16):
    result = jax.random.normal(stream_key, extent, jnp.float32) * width
    if len(shards) > 0:
        result = steps_of(stream_key, extent, shards, -0.22, 0.18) * result
    return jnp.clip(result, min=-most, max=most).astype(dtype)


def setup_inputs(seed: int = 0, part: int = 0) -> dict:
    key_of = jax.random.split(jax.random.key(seed), 10)
    own_keys = jax.random.split(jax.random.fold_in(key_of[9], part), 10)
    tokens = noise(own_keys[0], (IMAGES, SEQ, D), 1.0, 6.0, ((0, 16),))
    logits = draw_logits(jax.random.fold_in(jax.random.fold_in(key_of[9], part), 71), part)
    slot_out = noise(own_keys[2], (EXPERTS, IMAGES, D), 0.25, 1.5, ((0, 16),))
    slot_in = noise(own_keys[3], (EXPERTS, IMAGES, D), 1.0, 6.0, ((0, 16),))
    out_grad = noise(own_keys[4], (IMAGES, SEQ, D), 32.0, 192.0, ((0, 16),))
    router = noise(key_of[5], (EXPERTS, D), D ** -0.5, 0.21875)
    w_in = noise(key_of[6], (EXPERTS, D, FF), D ** -0.5, 0.21875, ((0, 16),))
    bias_in = noise(key_of[7], (EXPERTS, FF), 1.0, 5.0, ((0, 16),), jnp.float32)
    w_out = noise(key_of[8], (EXPERTS, FF, D), FF ** -0.5, 0.109375, ((0, 16),))
    return dict(tokens=tokens, logits=logits, slot_out=slot_out, slot_in=slot_in, out_grad=out_grad, router=router, w_in=w_in, bias_in=bias_in, w_out=w_out)


gelu_root = 0.7978845608028654
gelu_cubic = 0.044715


def gelu_slope(values):
    inner_arg = gelu_root * (values + gelu_cubic * values * values * values)
    tanh_val = jnp.tanh(inner_arg)
    return 0.5 * (1.0 + tanh_val) + 0.5 * values * (1.0 - tanh_val * tanh_val) * gelu_root * (1.0 + 3.0 * gelu_cubic * values * values)


def expert_backward(inputs):
    slot_rows, slot_grads, weight_in, bias_row, weight_out = inputs
    hidden_pre = jnp.dot(slot_rows, weight_in, preferred_element_type=jnp.float32) + bias_row
    hidden_grad = jnp.dot(slot_grads, weight_out.T, preferred_element_type=jnp.float32)
    pre_grad = (hidden_grad * gelu_slope(hidden_pre)).astype(jnp.bfloat16)
    return jnp.dot(pre_grad, weight_in.T, preferred_element_type=jnp.float32).astype(jnp.bfloat16)


def reference(tokens, logits, slot_out, slot_in, out_grad, router, w_in, bias_in, w_out):
    dispatch = jax.nn.softmax(logits, axis=1)
    combine = jax.nn.softmax(logits, axis=2)
    combine_rounded = combine.astype(jnp.bfloat16)
    dispatch_rounded = dispatch.astype(jnp.bfloat16)
    tokens_wide = tokens.astype(jnp.float32)
    grad_wide = out_grad.astype(jnp.float32)
    slot_grad = jnp.einsum("itj,itd->jid", combine_rounded.astype(jnp.float32), grad_wide).astype(jnp.bfloat16)
    slot_in_grad = lax.map(expert_backward, (slot_in, slot_grad, w_in, bias_in, w_out))
    in_grad_wide = slot_in_grad.astype(jnp.float32)
    combine_grad = jnp.einsum("itd,jid->itj", grad_wide, slot_out.astype(jnp.float32))
    comb_logit = (combine * (combine_grad - jnp.sum(combine * combine_grad, axis=2, keepdims=True))).astype(jnp.bfloat16)
    dispatch_grad = jnp.einsum("itd,jid->itj", tokens_wide, in_grad_wide)
    disp_logit = (dispatch * (dispatch_grad - jnp.sum(dispatch * dispatch_grad, axis=1, keepdims=True))).astype(jnp.bfloat16)
    router_wide = router.astype(jnp.float32)
    comb_wide = comb_logit.astype(jnp.float32)
    disp_wide = disp_logit.astype(jnp.float32)
    input_grad = jnp.einsum("itj,jid->itd", dispatch_rounded.astype(jnp.float32), in_grad_wide)
    input_grad = input_grad + jnp.einsum("itj,jd->itd", comb_wide, router_wide)
    input_grad = input_grad + jnp.einsum("itj,jd->itd", disp_wide, router_wide)
    router_grad = jnp.einsum("itj,itd->jd", comb_wide, tokens_wide) + jnp.einsum("itj,itd->jd", disp_wide, tokens_wide)
    router_grad = router_grad / IMAGES
    return input_grad.astype(jnp.bfloat16), router_grad
```

```python
import functools

import jax
import jax.numpy as jnp
from jax import lax
from jax.experimental import pallas as pl
from jax.experimental.pallas import tpu as pltpu
from jax.sharding import PartitionSpec as P

gelu_root = 0.7978845608028654
gelu_cubic = 0.044715
MESH = pl.DeviceIdType.MESH
F32 = jnp.float32
BF16 = jnp.bfloat16


def gelu_slope(values):
    square = values * values
    inner_arg = gelu_root * (values + gelu_cubic * square * values)
    tanh_val = jnp.tanh(inner_arg)
    return 0.5 * (1.0 + tanh_val) + 0.5 * values * (1.0 - tanh_val * tanh_val) * gelu_root * (
        1.0 + 3.0 * gelu_cubic * square
    )


def dot(a, b):
    return lax.dot_general(a, b, (((1,), (0,)), ((), ())), preferred_element_type=F32)


def dot_nt(a, b):
    return lax.dot_general(a, b, (((1,), (1,)), ((), ())), preferred_element_type=F32)


def dot_tn(a, b):
    return lax.dot_general(a, b, (((0,), (0,)), ((), ())), preferred_element_type=F32)


def ones_where(rows, cols, wanted):
    r = lax.broadcasted_iota(jnp.int32, (rows, cols), 0)
    c = lax.broadcasted_iota(jnp.int32, (rows, cols), 1)
    return jnp.where(wanted(r, c), 1.0, 0.0).astype(BF16)


def body(
    n, b, pad, chunk, tile, cuts,
    tok_hbm, log_hbm, so_hbm, si_hbm, og_hbm, rt_hbm, wi_hbm, bi_hbm, wo_hbm,
    ig_ref, rg_ref,
    tok, logv, so, si, og, rt, wi, bi, wo,
    comb, disp, combl, displ, slope, sg, sip, rsum, part, dgs,
    send_s, recv_s, send_a, recv_a, send_b, recv_b, send_r, recv_r, tok_t, pre, wi_t, wo_t,
    load_sem, sem_a, sem_s, sem_b, sem_r,
):
    me = lax.axis_index("exp")
    width = tok.shape[2]
    hidden = wi.shape[2]
    rows = n * b
    padded = n * pad

    barrier = pltpu.get_barrier_semaphore()

    def greet(d, _):
        peer = lax.rem(me + d, n)
        pl.semaphore_signal(barrier, inc=1, device_id={"exp": peer}, device_id_type=MESH)
        return 0

    lax.fori_loop(1, n, greet, 0, unroll=True)

    loads = {}
    pairs = [
        ("log", log_hbm, logv), ("og", og_hbm, og), ("si", si_hbm, si),
        ("wi", wi_hbm, wi), ("bi", bi_hbm, bi), ("wo", wo_hbm, wo), ("so", so_hbm, so), ("tok", tok_hbm, tok),
        ("rt", rt_hbm, rt),
    ]
    for at, (name, src, dst) in enumerate(pairs):
        loads[name] = pltpu.make_async_copy(src, dst, load_sem.at[at])
        loads[name].start()

    def view(ref, at, cut):
        rows_sent = min(b, ref.shape[1])
        return ref.at[at, :rows_sent, cut[0]:cut[1]]

    lone = jnp.abs(n - 1 - 2 * me)

    def far_first(k):
        pair = jnp.maximum(k - lone, 0)
        step = jnp.minimum(me, n - 1 - me) - pair // 2
        end = jnp.where(me < n // 2, n - 1 - k, k)
        return jnp.where(k < lone, end, me + step * (1 - 2 * (pair % 2)))

    def send_all(src, dst, sems, cut):
        def step(k, _):
            peer = far_first(k)
            pltpu.make_async_remote_copy(
                src_ref=view(src, peer, cut), dst_ref=view(dst, me, cut), send_sem=sems.at[0],
                recv_sem=sems.at[1], device_id={"exp": peer}, device_id_type=MESH,
            ).start()
            return 0

        lax.fori_loop(0, n - 1, step, 0, unroll=True)
        dst[me, :, cut[0]:cut[1]] = src[me, :, cut[0]:cut[1]]

    def everything(src, dst, sems, cut):
        return pltpu.make_async_remote_copy(
            src_ref=view(src, slice(0, n - 1), cut), dst_ref=view(dst, slice(0, n - 1), cut), send_sem=sems.at[0],
            recv_sem=sems.at[1], device_id={"exp": lax.rem(me + 1, n)}, device_id_type=MESH,
        )

    def wait_all(src, dst, sems, cut):
        everything(src, dst, sems, cut).wait_recv()

    def drain(src, dst, sems, cut):
        everything(src, dst, sems, cut).wait_send()

    whole = (0, width)
    spread = ones_where(padded, rows, lambda r, c: (r % pad < b) & (c == (r // pad) * b + r % pad))
    to_peers = ones_where(padded, rows, lambda r, c: (r % pad < b) & (c == (r % pad) * n + r // pad))
    to_images = ones_where(rows, padded, lambda r, c: c == (r % n) * pad + r // n)

    def grouped(x):
        return x.reshape(n, pad, x.shape[1]).astype(BF16)

    def flat(x):
        wide = x.astype(F32)
        if pad != b:
            wide = jnp.where(lax.broadcasted_iota(jnp.int32, (1, pad, 1), 1) < b, wide, 0.0)
        return wide.reshape(padded, x.shape[2]).astype(BF16)

    def of_image(i):
        return slice(i * n, (i + 1) * n)

    loads["log"].wait()
    for i in range(b):
        lt = logv[i]
        e = jnp.exp(lt - jnp.max(lt, axis=0, keepdims=True))
        comb[i] = e / jnp.sum(e, axis=0, keepdims=True)
    loads["og"].wait()
    for i in range(b):
        sg[of_image(i), :] = dot(comb[i].astype(BF16), og[i]).astype(BF16)
    send_a[...] = grouped(dot(to_peers, sg[...]))
    pl.semaphore_wait(barrier, n - 1)
    for q, cut in enumerate(cuts):
        send_all(send_a, recv_a, sem_a.at[q], cut)

    loads["si"].wait()
    sip[...] = dot(spread, si[0]).astype(BF16)
    loads["wi"].wait()
    loads["bi"].wait()
    for k in range(0, hidden, tile):
        hp = dot(sip[...], wi[0, :, k:k + tile]) + bi[:, k:k + tile]
        slope[:, k:k + tile] = gelu_slope(hp)
        wi_t[k:k + tile, :] = wi[0, :, k:k + tile].T
    for i in range(b):
        lt = logv[i]
        e = jnp.exp(lt - jnp.max(lt, axis=1, keepdims=True))
        disp[i] = e / jnp.sum(e, axis=1, keepdims=True)
    loads["so"].wait()
    send_s[...] = grouped(dot(spread, so[0]))
    send_all(send_s, recv_s, sem_s, whole)
    loads["wo"].wait()
    for k in range(0, hidden, chunk):
        wo_t[:, k:k + chunk] = wo[0, k:k + chunk, :].T

    for q, (lo, hi) in enumerate(cuts):
        wait_all(send_a, recv_a, sem_a.at[q], (lo, hi))
        got = flat(recv_a[:, :, lo:hi])
        for k in range(0, hidden, chunk):
            hg = dot(got, wo_t[lo:hi, k:k + chunk])
            if q > 0:
                hg = hg + part[:, k:k + chunk]
            if q < len(cuts) - 1:
                part[:, k:k + chunk] = hg
            else:
                pre[:, k:k + chunk] = (hg * slope[:, k:k + chunk]).astype(BF16)
    for q, (lo, hi) in enumerate(cuts):
        send_b[:, :, lo:hi] = grouped(dot(pre[...], wi_t[:, lo:hi]))
        send_all(send_b, recv_b, sem_b.at[q], (lo, hi))

    loads["tok"].wait()
    loads["rt"].wait()
    for i in range(b):
        tok_t[i] = tok[i].T
    wait_all(send_s, recv_s, sem_s, whole)
    outs = dot(to_images, flat(recv_s[...])).astype(BF16)
    for i in range(b):
        dgs[i] = dot_nt(outs[of_image(i), :], og[i])
    for i in range(b):
        c, cg = comb[i], dgs[i]
        combl[i] = (c * (cg - jnp.sum(c * cg, axis=0, keepdims=True))).astype(BF16)
    racc = jnp.zeros((n, width), F32)
    for i in range(b):
        racc = racc + dot(combl[i], tok[i])
    rsum[...] = racc

    for q, (lo, hi) in enumerate(cuts):
        wait_all(send_b, recv_b, sem_b.at[q], (lo, hi))
        sg[:, lo:hi] = dot(to_images, flat(recv_b[:, :, lo:hi])).astype(BF16)
        for i in range(b):
            dg = dot(sg[of_image(i), lo:hi], tok_t[i, lo:hi, :])
            dgs[i] = dg if q == 0 else dgs[i] + dg
    for i in range(b):
        d, dg = disp[i], dgs[i]
        displ[i] = (d * (dg - jnp.sum(d * dg, axis=1, keepdims=True))).astype(BF16)
    racc = rsum[...]
    for i in range(b):
        racc = racc + dot(displ[i], tok[i])
    send_r[...] = racc.reshape(n, 1, width)
    send_all(send_r, recv_r, sem_r, whole)

    for i in range(b):
        left = jnp.concatenate([disp[i].astype(BF16), combl[i], displ[i]], axis=0)
        right = jnp.concatenate([sg[of_image(i), :], rt[...], rt[...]], axis=0)
        ig_ref[i] = dot_tn(left, right).astype(BF16)

    drain(send_s, recv_s, sem_s, whole)
    for q, cut in enumerate(cuts):
        drain(send_a, recv_a, sem_a.at[q], cut)
        drain(send_b, recv_b, sem_b.at[q], cut)
    wait_all(send_r, recv_r, sem_r, whole)
    rg_ref[...] = jnp.sum(recv_r[...], axis=0) / rows
    drain(send_r, recv_r, sem_r, whole)


def write_out(ig_ref, rg_ref, ig_hbm, rg_hbm, sems):
    copies = [pltpu.make_async_copy(rg_ref, rg_hbm, sems.at[0])]
    for i in range(ig_ref.shape[0]):
        copies.append(pltpu.make_async_copy(ig_ref.at[i], ig_hbm.at[i], sems.at[i + 1]))
    for copy in copies:
        copy.start()
    for copy in copies:
        copy.wait()


def on_device(tokens, logits, slot_out, slot_in, out_grad, router, w_in, bias_in, w_out):
    b, seq, width = tokens.shape
    n = lax.axis_size("exp")
    hidden = w_in.shape[2]
    pad = -(-b // 8) * 8
    padded = n * pad
    chunk = 768 if hidden % 768 == 0 else hidden
    tile = 256 if hidden % 256 == 0 else hidden
    cuts = [(0, width - 256), (width - 256, width)] if width % 256 == 0 and width > 256 else [(0, width)]
    hbm_spec = pl.BlockSpec(memory_space=pltpu.HBM)
    vmem_spec = pl.BlockSpec(memory_space=pltpu.VMEM)
    limit = 67043328 - 65536 - b * (-(-seq // 8) * 8) * width * 2
    exchange = pltpu.VMEM((n, pad, width), BF16)
    small = pltpu.VMEM((n, 1, width), F32)
    sems = pltpu.SemaphoreType.DMA((2,))
    sems_cut = pltpu.SemaphoreType.DMA((len(cuts), 2))
    ig, rg = pl.pallas_call(
        functools.partial(body, n, b, pad, chunk, tile, cuts),
        out_shape=(
            pltpu.VMEM((b, seq, width), BF16),
            pltpu.VMEM((1, width), F32),
        ),
        in_specs=[hbm_spec] * 9,
        out_specs=(vmem_spec, vmem_spec),
        scratch_shapes=[
            pltpu.VMEM(tokens.shape, BF16),
            pltpu.VMEM((b, n, seq), F32),
            pltpu.VMEM(slot_out.shape, BF16),
            pltpu.VMEM(slot_in.shape, BF16),
            pltpu.VMEM(out_grad.shape, BF16),
            pltpu.VMEM(router.shape, BF16),
            pltpu.VMEM(w_in.shape, BF16),
            pltpu.VMEM(bias_in.shape, F32),
            pltpu.VMEM(w_out.shape, BF16),
            pltpu.VMEM((b, n, seq), F32),
            pltpu.VMEM((b, n, seq), F32),
            pltpu.VMEM((b, n, seq), BF16),
            pltpu.VMEM((b, n, seq), BF16),
            pltpu.VMEM((padded, hidden), F32),
            pltpu.VMEM((n * b, width), BF16),
            pltpu.VMEM((padded, width), BF16),
            pltpu.VMEM((n, width), F32),
            pltpu.VMEM((padded, hidden), F32),
            pltpu.VMEM((b, n, seq), F32),
            exchange, exchange, exchange, exchange, exchange, exchange, small, small,
            pltpu.VMEM((b, width, seq), BF16),
            pltpu.VMEM((padded, hidden), BF16),
            pltpu.VMEM((hidden, width), BF16),
            pltpu.VMEM((width, hidden), BF16),
            pltpu.SemaphoreType.DMA((9,)),
            sems_cut, sems, sems_cut, sems,
        ],
        compiler_params=pltpu.CompilerParams(
            collective_id=0, has_side_effects=True, vmem_limit_bytes=limit
        ),
        name="moe_input_grad",
    )(tokens, jnp.swapaxes(logits, 1, 2), slot_out, slot_in, out_grad, router, w_in, bias_in, w_out)
    return pl.pallas_call(
        write_out,
        out_shape=(jax.ShapeDtypeStruct(ig.shape, BF16), jax.ShapeDtypeStruct(rg.shape, F32)),
        in_specs=[vmem_spec, vmem_spec],
        out_specs=(hbm_spec, hbm_spec),
        scratch_shapes=[pltpu.SemaphoreType.DMA((b + 1,))],
        compiler_params=pltpu.CompilerParams(vmem_limit_bytes=1 << 20),
        name="write_out",
    )(
        pltpu.with_memory_space_constraint(ig, pltpu.VMEM),
        pltpu.with_memory_space_constraint(rg, pltpu.VMEM),
    )


def solution(mesh):
    placed = (
        P(("grp", "exp"), None, None),
        P(("grp", "exp"), None, None),
        P(("grp", "exp"), None, None),
        P(("grp", "exp"), None, None),
        P(("grp", "exp"), None, None),
        P(),
        P("exp", None, None),
        P("exp", None),
        P("exp", None, None),
    )
    return jax.shard_map(
        on_device,
        mesh=mesh,
        in_specs=placed,
        out_specs=(P(("grp", "exp"), None, None), P(("grp", "exp"), None)),
        check_vma=False,
    )
```

```python
import functools

import jax
import jax.numpy as jnp
from jax import lax
from jax.experimental import pallas as pl
from jax.experimental.pallas import tpu as pltpu
from jax.sharding import PartitionSpec as P

gelu_root = 0.7978845608028654
gelu_cubic = 0.044715
MESH = pl.DeviceIdType.MESH
F32 = jnp.float32
BF16 = jnp.bfloat16


def gelu_slope(values):
    square = values * values
    inner_arg = gelu_root * (values + gelu_cubic * square * values)
    tanh_val = jnp.tanh(inner_arg)
    return 0.5 * (1.0 + tanh_val) + 0.5 * values * (1.0 - tanh_val * tanh_val) * gelu_root * (
        1.0 + 3.0 * gelu_cubic * square
    )


def dot(a, b):
    return lax.dot_general(a, b, (((1,), (0,)), ((), ())), preferred_element_type=F32)


def dot_nt(a, b):
    return lax.dot_general(a, b, (((1,), (1,)), ((), ())), preferred_element_type=F32)


def dot_tn(a, b):
    return lax.dot_general(a, b, (((0,), (0,)), ((), ())), preferred_element_type=F32)


def ones_where(rows, cols, wanted):
    r = lax.broadcasted_iota(jnp.int32, (rows, cols), 0)
    c = lax.broadcasted_iota(jnp.int32, (rows, cols), 1)
    return jnp.where(wanted(r, c), 1.0, 0.0).astype(BF16)


def body(
    n, b, pad, chunk, tile, cuts,
    tok_hbm, log_hbm, so_hbm, si_hbm, og_hbm, rt_hbm, wi_hbm, bi_hbm, wo_hbm,
    ig_ref, rg_ref,
    tok, logv, so, si, og, rt, wi, bi, wo,
    comb, disp, combl, displ_a, displ_b, slope, sg, sig_a, sig_b, sip, rsum, part, dgs,
    send_s, recv_s, send_a, recv_a, send_b, recv_b, send_r, recv_r, tok_t, pre, wi_t, wo_t,
    load_sem, sem_a, sem_s, sem_b, sem_r,
):
    me = lax.axis_index("exp")
    width = tok.shape[2]
    hidden = wi.shape[2]
    rows = n * b
    padded = n * pad
    sig, displ = (sig_a, sig_b), (displ_a, displ_b)
    groups = [(0, n // 4, -(-(n // 4) // 8) * 8), (n // 4, n, n)]

    barrier = pltpu.get_barrier_semaphore()

    def greet(d, _):
        peer = lax.rem(me + d, n)
        pl.semaphore_signal(barrier, inc=1, device_id={"exp": peer}, device_id_type=MESH)
        return 0

    lax.fori_loop(1, n, greet, 0, unroll=True)

    loads = {}
    pairs = [
        ("log", log_hbm, logv), ("og", og_hbm, og), ("si", si_hbm, si),
        ("wi", wi_hbm, wi), ("bi", bi_hbm, bi), ("wo", wo_hbm, wo), ("so", so_hbm, so), ("tok", tok_hbm, tok),
        ("rt", rt_hbm, rt),
    ]
    for at, (name, src, dst) in enumerate(pairs):
        loads[name] = pltpu.make_async_copy(src, dst, load_sem.at[at])
        loads[name].start()

    def view(ref, at, cut):
        rows_sent = min(b, ref.shape[1])
        return ref.at[at, :rows_sent, cut[0]:cut[1]]

    g = 4 if n % 4 == 0 else 1
    block = me // g
    lone = jnp.abs(n // g - 1 - 2 * block)

    def far_first(k):
        kb, w = k // g, k % g
        if k >= n - g:
            return me ^ (g - 1 - w)
        pair = jnp.maximum(kb - lone, 0)
        step = jnp.minimum(block, n // g - 1 - block) - pair // 2
        end = jnp.where(block < n // g // 2, n // g - 1 - kb, kb)
        there = jnp.where(kb < lone, end, block + step * (1 - 2 * (pair % 2)))
        return there * g + ((me % g) ^ (g - 1 - w))

    def send_all(src, dst, sems, cut, first=0, last=n - 1):
        for k in range(first, last):
            peer = far_first(k)
            pltpu.make_async_remote_copy(
                src_ref=view(src, peer, cut), dst_ref=view(dst, me, cut), send_sem=sems.at[0],
                recv_sem=sems.at[1], device_id={"exp": peer}, device_id_type=MESH,
            ).start()
        if last == n - 1:
            dst[me, :, cut[0]:cut[1]] = src[me, :, cut[0]:cut[1]]

    def everything(src, dst, sems, cut):
        return pltpu.make_async_remote_copy(
            src_ref=view(src, slice(0, n - 1), cut), dst_ref=view(dst, slice(0, n - 1), cut), send_sem=sems.at[0],
            recv_sem=sems.at[1], device_id={"exp": lax.rem(me + 1, n)}, device_id_type=MESH,
        )

    def wait_all(src, dst, sems, cut):
        everything(src, dst, sems, cut).wait_recv()

    def drain(src, dst, sems, cut):
        everything(src, dst, sems, cut).wait_send()

    whole = (0, width)
    spread = ones_where(padded, rows, lambda r, c: (r % pad < b) & (c == (r // pad) * b + r % pad))
    to_peers = ones_where(padded, rows, lambda r, c: (r % pad < b) & (c == (r % pad) * n + r // pad))
    to_images = ones_where(rows, padded, lambda r, c: c == (r % n) * pad + r // n)

    def grouped(x):
        return x.reshape(n, pad, x.shape[1]).astype(BF16)

    def flat(x):
        wide = x.astype(F32)
        if pad != b:
            wide = jnp.where(lax.broadcasted_iota(jnp.int32, (1, pad, 1), 1) < b, wide, 0.0)
        return wide.reshape(x.shape[0] * pad, x.shape[2]).astype(BF16)

    def of_image(i):
        return slice(i * n, (i + 1) * n)

    loads["log"].wait()
    for i in range(b):
        lt = logv[i]
        e = jnp.exp(lt - jnp.max(lt, axis=0, keepdims=True))
        comb[i] = e / jnp.sum(e, axis=0, keepdims=True)
    loads["og"].wait()
    for i in range(b):
        sg[of_image(i), :] = dot(comb[i].astype(BF16), og[i]).astype(BF16)
    send_a[...] = grouped(dot(to_peers, sg[...]))
    pl.semaphore_wait(barrier, n - 1)
    for q, cut in enumerate(cuts):
        send_all(send_a, recv_a, sem_a.at[q], cut, 0, n // 4)
    for q, cut in enumerate(cuts):
        send_all(send_a, recv_a, sem_a.at[q], cut, n // 4)

    loads["si"].wait()
    sip[...] = dot(spread, si[0]).astype(BF16)
    loads["wi"].wait()
    loads["bi"].wait()
    for k in range(0, hidden, tile):
        hp = dot(sip[...], wi[0, :, k:k + tile]) + bi[:, k:k + tile]
        slope[:, k:k + tile] = gelu_slope(hp)
        wi_t[k:k + tile, :] = wi[0, :, k:k + tile].T
    for i in range(b):
        lt = logv[i]
        e = jnp.exp(lt - jnp.max(lt, axis=1, keepdims=True))
        disp[i] = e / jnp.sum(e, axis=1, keepdims=True)
    loads["so"].wait()
    send_s[...] = grouped(dot(spread, so[0]))
    send_all(send_s, recv_s, sem_s, whole)
    loads["wo"].wait()
    for k in range(0, hidden, chunk):
        wo_t[:, k:k + chunk] = wo[0, k:k + chunk, :].T

    for q, (lo, hi) in enumerate(cuts):
        wait_all(send_a, recv_a, sem_a.at[q], (lo, hi))
        got = flat(recv_a[:, :, lo:hi])
        for k in range(0, hidden, chunk):
            hg = dot(got, wo_t[lo:hi, k:k + chunk])
            if q > 0:
                hg = hg + part[:, k:k + chunk]
            if q < len(cuts) - 1:
                part[:, k:k + chunk] = hg
            else:
                pre[:, k:k + chunk] = (hg * slope[:, k:k + chunk]).astype(BF16)
    mine = jnp.minimum(me // groups[0][1], 1)

    def send_rows(q, ks):
        lo, hi = cuts[q]
        for k in ks:
            peer = far_first(k)
            pltpu.make_async_remote_copy(
                src_ref=send_b.at[peer, :b, lo:hi], dst_ref=recv_b.at[me, :b, lo:hi], send_sem=sem_b.at[q, 0],
                recv_sem=sem_b.at[q, 1 + mine], device_id={"exp": peer}, device_id_type=MESH,
            ).start()

    def rows_between(q, own):
        lo, hi = cuts[q]
        return pltpu.make_async_remote_copy(
            src_ref=send_b.at[own, :b, lo:hi], dst_ref=recv_b.at[own, :b, lo:hi], send_sem=sem_b.at[q, 0],
            recv_sem=sem_b.at[q, 1 + (own.start > 0)], device_id={"exp": lax.rem(me + 1, n)}, device_id_type=MESH,
        )

    for q, (lo, hi) in enumerate(cuts):
        send_b[:, :, lo:hi] = grouped(dot(pre[...], wi_t[:, lo:hi]))
        send_rows(q, range(n // 4))
        pltpu.make_async_copy(
            send_b.at[me, :b, lo:hi], recv_b.at[me, :b, lo:hi], sem_b.at[q, 1 + mine]
        ).start()
    for k in range(n // 4, n - 1):
        for q in range(len(cuts)):
            send_rows(q, [k])

    loads["tok"].wait()
    loads["rt"].wait()
    for i in range(b):
        tok_t[i] = tok[i].T
    wait_all(send_s, recv_s, sem_s, whole)
    outs = dot(to_images, flat(recv_s[...])).astype(BF16)
    for i in range(b):
        dgs[i] = dot_nt(outs[of_image(i), :], og[i])
    for i in range(b):
        c, cg = comb[i], dgs[i]
        combl[i] = (c * (cg - jnp.sum(c * cg, axis=0, keepdims=True))).astype(BF16)
    racc = jnp.zeros((n, width), F32)
    for i in range(b):
        racc = racc + dot(combl[i], tok[i])
    rsum[...] = racc

    for h, (lo, hi, tall) in enumerate(groups):
        own = slice(lo, hi)
        first = tall - (hi - lo) if h else 0
        to_group = ones_where(
            b * tall, (hi - lo) * pad,
            lambda r, c: (c == (r % tall - first) * pad + r // tall) & (r % tall >= first) & (r % tall < first + hi - lo),
        )
        for q, (left, right) in enumerate(cuts):
            rows_between(q, own).wait_recv()
            got = dot(to_group, flat(recv_b[own, :, left:right]))
            sig[h][:, :, left:right] = got.reshape(b, tall, right - left).astype(BF16)
            for i in range(b):
                dg = dot(sig[h][i, :, left:right], tok_t[i, left:right, :])
                dgs[i, :tall, :] = dg if q == 0 else dgs[i, :tall, :] + dg
        racc = rsum[:tall, :]
        for i in range(b):
            d, dg = disp[i, :tall, :], dgs[i, :tall, :]
            dl = (d * (dg - jnp.sum(d * dg, axis=1, keepdims=True))).astype(BF16)
            displ[h][i] = dl
            racc = racc + dot(dl, tok[i])
        send_r[own] = racc[lo:hi].reshape(hi - lo, 1, width)
        for j in range(lo, hi):
            @pl.when(me != j)
            def _():
                pltpu.make_async_remote_copy(
                    src_ref=send_r.at[j], dst_ref=recv_r.at[me], send_sem=sem_r.at[0],
                    recv_sem=sem_r.at[1], device_id={"exp": j}, device_id_type=MESH,
                ).start()
    recv_r[me] = send_r[me]

    for i in range(b):
        tall = groups[0][2]
        dr = disp[i].astype(BF16)
        left = jnp.concatenate([dr, combl[i], displ[1][i], dr[:tall], displ[0][i]], axis=0)
        right = jnp.concatenate([sig[1][i], rt[...], rt[...], sig[0][i], rt[:tall, :]], axis=0)
        ig_ref[i] = dot_tn(left, right).astype(BF16)

    drain(send_s, recv_s, sem_s, whole)
    for q, cut in enumerate(cuts):
        drain(send_a, recv_a, sem_a.at[q], cut)
    for q in range(len(cuts)):
        rows_between(q, slice(0, n - 1)).wait_send()
    wait_all(send_r, recv_r, sem_r, whole)
    rg_ref[...] = jnp.sum(recv_r[...], axis=0) / rows
    drain(send_r, recv_r, sem_r, whole)


def write_out(ig_ref, rg_ref, ig_hbm, rg_hbm, sems):
    copies = [pltpu.make_async_copy(rg_ref, rg_hbm, sems.at[0])]
    for i in range(ig_ref.shape[0]):
        copies.append(pltpu.make_async_copy(ig_ref.at[i], ig_hbm.at[i], sems.at[i + 1]))
    for copy in copies:
        copy.start()
    for copy in copies:
        copy.wait()


def on_device(tokens, logits, slot_out, slot_in, out_grad, router, w_in, bias_in, w_out):
    b, seq, width = tokens.shape
    n = lax.axis_size("exp")
    hidden = w_in.shape[2]
    pad = -(-b // 8) * 8
    padded = n * pad
    early = -(-(n // 4) // 8) * 8
    chunk = 768 if hidden % 768 == 0 else hidden
    tile = 256 if hidden % 256 == 0 else hidden
    cuts = [(0, width - 256), (width - 256, width)] if width % 256 == 0 and width > 256 else [(0, width)]
    hbm_spec = pl.BlockSpec(memory_space=pltpu.HBM)
    vmem_spec = pl.BlockSpec(memory_space=pltpu.VMEM)
    limit = 67043328 - 65536 - b * (-(-seq // 8) * 8) * width * 2
    exchange = pltpu.VMEM((n, pad, width), BF16)
    small = pltpu.VMEM((n, 1, width), F32)
    sems = pltpu.SemaphoreType.DMA((2,))
    sems_cut = pltpu.SemaphoreType.DMA((2, 2))
    ig, rg = pl.pallas_call(
        functools.partial(body, n, b, pad, chunk, tile, cuts),
        out_shape=(
            pltpu.VMEM((b, seq, width), BF16),
            pltpu.VMEM((1, width), F32),
        ),
        in_specs=[hbm_spec] * 9,
        out_specs=(vmem_spec, vmem_spec),
        scratch_shapes=[
            pltpu.VMEM(tokens.shape, BF16),
            pltpu.VMEM((b, n, seq), F32),
            pltpu.VMEM(slot_out.shape, BF16),
            pltpu.VMEM(slot_in.shape, BF16),
            pltpu.VMEM(out_grad.shape, BF16),
            pltpu.VMEM(router.shape, BF16),
            pltpu.VMEM(w_in.shape, BF16),
            pltpu.VMEM(bias_in.shape, F32),
            pltpu.VMEM(w_out.shape, BF16),
            pltpu.VMEM((b, n, seq), F32),
            pltpu.VMEM((b, n, seq), F32),
            pltpu.VMEM((b, n, seq), BF16),
            pltpu.VMEM((b, early, seq), BF16),
            pltpu.VMEM((b, n, seq), BF16),
            pltpu.VMEM((padded, hidden), F32),
            pltpu.VMEM((n * b, width), BF16),
            pltpu.VMEM((b, early, width), BF16),
            pltpu.VMEM((b, n, width), BF16),
            pltpu.VMEM((padded, width), BF16),
            pltpu.VMEM((n, width), F32),
            pltpu.VMEM((padded, hidden), F32),
            pltpu.VMEM((b, n, seq), F32),
            exchange, exchange, exchange, exchange, exchange, exchange, small, small,
            pltpu.VMEM((b, width, seq), BF16),
            pltpu.VMEM((padded, hidden), BF16),
            pltpu.VMEM((hidden, width), BF16),
            pltpu.VMEM((width, hidden), BF16),
            pltpu.SemaphoreType.DMA((9,)),
            sems_cut, sems, pltpu.SemaphoreType.DMA((len(cuts), 3)), sems,
        ],
        compiler_params=pltpu.CompilerParams(
            collective_id=0, has_side_effects=True, vmem_limit_bytes=limit
        ),
        name="moe_input_grad",
    )(tokens, jnp.swapaxes(logits, 1, 2), slot_out, slot_in, out_grad, router, w_in, bias_in, w_out)
    return pl.pallas_call(
        write_out,
        out_shape=(jax.ShapeDtypeStruct(ig.shape, BF16), jax.ShapeDtypeStruct(rg.shape, F32)),
        in_specs=[vmem_spec, vmem_spec],
        out_specs=(hbm_spec, hbm_spec),
        scratch_shapes=[pltpu.SemaphoreType.DMA((b + 1,))],
        compiler_params=pltpu.CompilerParams(vmem_limit_bytes=1 << 20),
        name="write_out",
    )(
        pltpu.with_memory_space_constraint(ig, pltpu.VMEM),
        pltpu.with_memory_space_constraint(rg, pltpu.VMEM),
    )


def solution(mesh):
    placed = (
        P(("grp", "exp"), None, None),
        P(("grp", "exp"), None, None),
        P(("grp", "exp"), None, None),
        P(("grp", "exp"), None, None),
        P(("grp", "exp"), None, None),
        P(),
        P("exp", None, None),
        P("exp", None),
        P("exp", None, None),
    )
    return jax.shard_map(
        on_device,
        mesh=mesh,
        in_specs=placed,
        out_specs=(P(("grp", "exp"), None, None), P(("grp", "exp"), None)),
        check_vma=False,
    )
```

```python
import functools

import jax
import jax.numpy as jnp
from jax import lax
from jax.experimental import pallas as pl
from jax.experimental.pallas import tpu as pltpu
from jax.sharding import PartitionSpec as P

gelu_root = 0.7978845608028654
gelu_cubic = 0.044715
MESH = pl.DeviceIdType.MESH
F32 = jnp.float32
BF16 = jnp.bfloat16


def gelu_slope(values):
    square = values * values
    inner_arg = gelu_root * (values + gelu_cubic * square * values)
    tanh_val = jnp.tanh(inner_arg)
    return 0.5 * (1.0 + tanh_val) + 0.5 * values * (1.0 - tanh_val * tanh_val) * gelu_root * (
        1.0 + 3.0 * gelu_cubic * square
    )


def dot(a, b):
    return lax.dot_general(a, b, (((1,), (0,)), ((), ())), preferred_element_type=F32)


def dot_nt(a, b):
    return lax.dot_general(a, b, (((1,), (1,)), ((), ())), preferred_element_type=F32)


def dot_tn(a, b):
    return lax.dot_general(a, b, (((0,), (0,)), ((), ())), preferred_element_type=F32)


def ones_where(rows, cols, wanted):
    r = lax.broadcasted_iota(jnp.int32, (rows, cols), 0)
    c = lax.broadcasted_iota(jnp.int32, (rows, cols), 1)
    return jnp.where(wanted(r, c), 1.0, 0.0).astype(BF16)


def body(
    n, b, pad, chunk, tile, cuts,
    tok_hbm, log_hbm, so_hbm, si_hbm, og_hbm, rt_hbm, wi_hbm, bi_hbm, wo_hbm,
    ig_ref, rg_ref,
    tok, logv, so, si, og, rt, wi, bi, wo,
    comb, disp, combl, displ_a, displ_b, spread_disp, spread_dg, slope, sg, sig_a, sig_b, sip, rsum, part, dgs,
    send_s, recv_s, send_a, recv_a, send_b, recv_b, send_r, recv_r, tok_t, pre, wi_t, wo_t,
    load_sem, og_sem, sem_a, sem_s, sem_b, sem_r,
):
    me = lax.axis_index("exp")
    width = tok.shape[2]
    hidden = wi.shape[2]
    rows = n * b
    padded = n * pad
    lanes = 128
    seq = logv.shape[2]
    span = tok_t.shape[1] // b
    early = n // 4
    tall = early * pad

    barrier = pltpu.get_barrier_semaphore()

    def greet(d, _):
        peer = lax.rem(me + d, n)
        pl.semaphore_signal(barrier, inc=1, device_id={"exp": peer}, device_id_type=MESH)
        return 0

    def greet_all():
        lax.fori_loop(1, n, greet, 0, unroll=True)

    loads = {}
    pairs = [
        ("log", log_hbm, logv), ("og", og_hbm, og), ("si", si_hbm, si),
        ("wi", wi_hbm, wi), ("bi", bi_hbm, bi), ("wo", wo_hbm, wo), ("so", so_hbm, so), ("tok", tok_hbm, tok),
        ("rt", rt_hbm, rt),
    ]
    for at, (name, src, dst) in enumerate(pairs):
        loads[name] = pltpu.make_async_copy(src, dst, load_sem.at[at])
        if name == "og":
            for i in range(b):
                loads["og", i] = pltpu.make_async_copy(src.at[i], dst.at[i], og_sem.at[i])
                loads["og", i].start()
            continue
        if at == 2:
            greet_all()
        if name not in ("wo", "tok", "so", "rt"):
            loads[name].start()
    if span != seq:
        for i in range(b):
            tok_t[:, i * span + seq // lanes * lanes:(i + 1) * span] = jnp.zeros(
                (width, span - seq // lanes * lanes), BF16
            )

    def view(ref, at, cut):
        rows_sent = min(b, ref.shape[1])
        return ref.at[at, :rows_sent, cut[0]:cut[1]]

    g = 4 if n % 4 == 0 else 1
    block = me // g

    def peer_at(k):
        kb, w = k // g, k % g
        if k >= n - g:
            return me ^ (g - 1 - w)
        last = n // g - 1 - kb
        there = jnp.where(last + 1 > block, last + 1, last) if kb else 0
        there = jnp.where(block == 0, last, there)
        return there * g + ((me % g) ^ (g - 1 - w))

    def send_all(src, dst, sems, cut, first=0, last=n - 1):
        for k in range(first, last):
            peer = peer_at(k)
            pltpu.make_async_remote_copy(
                src_ref=view(src, peer, cut), dst_ref=view(dst, me, cut), send_sem=sems.at[0],
                recv_sem=sems.at[1], device_id={"exp": peer}, device_id_type=MESH,
            ).start()
        if last == n - 1:
            dst[me, :, cut[0]:cut[1]] = src[me, :, cut[0]:cut[1]]

    def everything(src, dst, sems, cut):
        return pltpu.make_async_remote_copy(
            src_ref=view(src, slice(0, n - 1), cut), dst_ref=view(dst, slice(0, n - 1), cut), send_sem=sems.at[0],
            recv_sem=sems.at[1], device_id={"exp": lax.rem(me + 1, n)}, device_id_type=MESH,
        )

    def wait_all(src, dst, sems, cut):
        everything(src, dst, sems, cut).wait_recv()

    def drain(src, dst, sems, cut):
        everything(src, dst, sems, cut).wait_send()

    whole = (0, width)
    spread = ones_where(padded, rows, lambda r, c: (r % pad < b) & (c == (r // pad) * b + r % pad))
    to_images = ones_where(rows, padded, lambda r, c: c == (r % n) * pad + r // n)

    def grouped(x):
        return x.reshape(n, pad, x.shape[1]).astype(BF16)

    def flat(x):
        wide = x.astype(F32)
        if pad != b:
            wide = jnp.where(lax.broadcasted_iota(jnp.int32, (1, pad, 1), 1) < b, wide, 0.0)
        return wide.reshape(x.shape[0] * pad, x.shape[2]).astype(BF16)

    def of_image(i):
        return slice(i * n, (i + 1) * n)

    loads["log"].wait()
    loads["wo"].start()
    loads["tok"].start()
    loads["so"].start()
    loads["rt"].start()
    for i in range(b):
        lt = logv[i]
        e = jnp.exp(lt - jnp.max(lt, axis=0, keepdims=True))
        comb[i] = e / jnp.sum(e, axis=0, keepdims=True)
    for i in range(b):
        loads["og", i].wait()
    for i in range(b):
        row = dot(comb[i].astype(BF16), og[i])
        for c in range(width // lanes):
            sg[c, pl.ds(i, n, stride=pad), :] = row[:, c * lanes:(c + 1) * lanes]
    for c in range(width // lanes):
        send_a[:, :, c * lanes:(c + 1) * lanes] = grouped(sg[c])
    def prepare():
        loads["si"].wait()
        sip[...] = dot(spread, si[0]).astype(BF16)
        loads["wi"].wait()
        loads["bi"].wait()
        for k in range(0, hidden, tile):
            hp = dot(sip[...], wi[0, :, k:k + tile]) + bi[:, k:k + tile]
            slope[:, k:k + tile] = gelu_slope(hp)
            wi_t[k:k + tile, :] = wi[0, :, k:k + tile].T

    pl.when(me < n // 8)(prepare)
    pl.semaphore_wait(barrier, n - 1)
    for q, cut in enumerate(cuts):
        send_all(send_a, recv_a, sem_a.at[q], cut, 0, n // 4)
    for q, cut in enumerate(cuts):
        send_all(send_a, recv_a, sem_a.at[q], cut, n // 4)

    pl.when(me >= n // 8)(prepare)

    for i in range(b):
        lt = logv[i]
        e = jnp.exp(lt - jnp.max(lt, axis=1, keepdims=True))
        disp[i] = e / jnp.sum(e, axis=1, keepdims=True)
    def send_slots():
        loads["so"].wait()
        send_s[...] = grouped(dot(spread, so[0]))
        send_all(send_s, recv_s, sem_s, whole)

    pl.when(me >= n // 8)(send_slots)
    loads["wo"].wait()
    for k in range(0, hidden, chunk):
        wo_t[:, k:k + chunk] = wo[0, k:k + chunk, :].T

    def turn_tokens():
        loads["tok"].wait()
        loads["rt"].wait()
        for i in range(b):
            tok_t[:, i * span:i * span + seq] = tok[i].T
        spread_disp[...] = jnp.zeros_like(spread_disp)
        for i in range(b):
            here = lax.broadcasted_iota(jnp.int32, (pad, seq), 0) == i
            for j in range(early):
                value = jnp.where(here, disp[i, j:j + 1, :], 0.0)
                spread_disp[j * pad:(j + 1) * pad, i * span:i * span + seq] = value

    pl.when(me < n // 8)(turn_tokens)
    pl.when(me < n // 8)(send_slots)
    for q, (lo, hi) in enumerate(cuts):
        wait_all(send_a, recv_a, sem_a.at[q], (lo, hi))
        got = flat(recv_a[:, :, lo:hi])
        for k in range(0, hidden, chunk):
            hg = dot(got, wo_t[lo:hi, k:k + chunk])
            if q > 0:
                hg = hg + part[:, k:k + chunk]
            if q < len(cuts) - 1:
                part[:, k:k + chunk] = hg
            else:
                pre[:, k:k + chunk] = (hg * slope[:, k:k + chunk]).astype(BF16)
    mine = jnp.minimum(me // early, 1)

    def send_rows(q, ks):
        lo, hi = cuts[q]
        for k in ks:
            peer = peer_at(k)
            pltpu.make_async_remote_copy(
                src_ref=send_b.at[peer, :b, lo:hi], dst_ref=recv_b.at[me, :b, lo:hi], send_sem=sem_b.at[q, 0],
                recv_sem=sem_b.at[q, 1 + mine], device_id={"exp": peer}, device_id_type=MESH,
            ).start()

    def rows_between(q, own):
        lo, hi = cuts[q]
        return pltpu.make_async_remote_copy(
            src_ref=send_b.at[own, :b, lo:hi], dst_ref=recv_b.at[own, :b, lo:hi], send_sem=sem_b.at[q, 0],
            recv_sem=sem_b.at[q, 1 + (own.start > 0)], device_id={"exp": lax.rem(me + 1, n)}, device_id_type=MESH,
        )

    for q, (lo, hi) in enumerate(cuts):
        send_b[:, :, lo:hi] = grouped(dot(pre[...], wi_t[:, lo:hi]))
        send_rows(q, range(n // 4))
        pltpu.make_async_copy(
            send_b.at[me, :b, lo:hi], recv_b.at[me, :b, lo:hi], sem_b.at[q, 1 + mine]
        ).start()
    for k in range(n // 4, n - 1):
        for q in range(len(cuts)):
            send_rows(q, [k])

    pl.when(me >= n // 8)(turn_tokens)
    wait_all(send_s, recv_s, sem_s, whole)
    outs = dot(to_images, flat(recv_s[...])).astype(BF16)
    for i in range(b):
        dgs[i] = dot_nt(outs[of_image(i), :], og[i])
    for i in range(b):
        c, cg = comb[i], dgs[i]
        combl[i] = (c * (cg - jnp.sum(c * cg, axis=0, keepdims=True))).astype(BF16)

    def send_router(lo, hi):
        for j in range(lo, hi):
            @pl.when(me != j)
            def _():
                pltpu.make_async_remote_copy(
                    src_ref=send_r.at[j], dst_ref=recv_r.at[me], send_sem=sem_r.at[0],
                    recv_sem=sem_r.at[1], device_id={"exp": j}, device_id_type=MESH,
                ).start()

    for q, (lo, hi) in enumerate(cuts):
        rows_between(q, slice(0, early)).wait_recv()
        got = flat(recv_b[:early, :, lo:hi])
        sig_a[:, lo:hi] = got
        dg = dot(got, tok_t[lo:hi, :])
        if q > 0:
            dg = dg + spread_dg[...]
        if q < len(cuts) - 1:
            spread_dg[...] = dg
    d = spread_disp[...]
    part_sum = d * dg
    dl = (part_sum - d * jnp.sum(part_sum, axis=1, keepdims=True)).astype(BF16)
    displ_a[...] = dl
    racc = jnp.zeros((n + tall, width), F32)
    for i in range(b):
        terms = jnp.concatenate([combl[i], dl[:, i * span:i * span + seq]], axis=0)
        racc = racc + dot(terms, tok[i])
    rsum[...] = racc[:n]
    own = jnp.sum(racc[n:].reshape(early, pad, width), axis=1, keepdims=True)
    send_r[:early] = own + racc[:early].reshape(early, 1, width)
    send_router(0, early)

    to_image_rows = ones_where(
        rows, (n - early) * pad,
        lambda r, c: (c == (r % n - early) * pad + r // n) & (r % n >= early),
    )
    for q, (lo, hi) in enumerate(cuts):
        rows_between(q, slice(early, n)).wait_recv()
        sig_b[:, lo:hi] = dot(to_image_rows, flat(recv_b[early:, :, lo:hi])).astype(BF16)
        for i in range(b):
            dg = dot(sig_b[of_image(i), lo:hi], tok_t[lo:hi, i * span:i * span + seq])
            dgs[i] = dg if q == 0 else dgs[i] + dg
    racc = rsum[...]
    for i in range(b):
        d, dg = disp[i], dgs[i]
        dl = (d * (dg - jnp.sum(d * dg, axis=1, keepdims=True))).astype(BF16)
        displ_b[i] = dl
        racc = racc + dot(dl, tok[i])
    send_r[early:] = racc[early:].reshape(n - early, 1, width)
    send_router(early, n)
    recv_r[me] = send_r[me]

    spread_rt = dot(
        ones_where(tall, n, lambda r, c: c == r // pad), rt[...]
    ).astype(BF16)
    for i in range(b):
        at = slice(i * span, i * span + seq)
        left = jnp.concatenate(
            [spread_disp[:, at].astype(BF16), displ_a[:, at], disp[i].astype(BF16), combl[i], displ_b[i]], axis=0
        )
        right = jnp.concatenate(
            [sig_a[...], spread_rt, sig_b[of_image(i), :], rt[...], rt[...]], axis=0
        )
        ig_ref[i] = dot_tn(left, right).astype(BF16)

    drain(send_s, recv_s, sem_s, whole)
    for q, cut in enumerate(cuts):
        drain(send_a, recv_a, sem_a.at[q], cut)
    for q in range(len(cuts)):
        rows_between(q, slice(0, n - 1)).wait_send()
    wait_all(send_r, recv_r, sem_r, whole)
    rg_ref[...] = jnp.sum(recv_r[...], axis=0) / rows
    drain(send_r, recv_r, sem_r, whole)


def write_out(ig_ref, rg_ref, ig_hbm, rg_hbm, sems):
    copies = [pltpu.make_async_copy(rg_ref, rg_hbm, sems.at[0])]
    for i in range(ig_ref.shape[0]):
        copies.append(pltpu.make_async_copy(ig_ref.at[i], ig_hbm.at[i], sems.at[i + 1]))
    for copy in copies:
        copy.start()
    for copy in copies:
        copy.wait()


def on_device(tokens, logits, slot_out, slot_in, out_grad, router, w_in, bias_in, w_out):
    b, seq, width = tokens.shape
    n = lax.axis_size("exp")
    hidden = w_in.shape[2]
    pad = -(-b // 8) * 8
    padded = n * pad
    tall = n // 4 * pad
    span = -(-seq // 128) * 128
    chunk = 768 if hidden % 768 == 0 else hidden
    tile = 256 if hidden % 256 == 0 else hidden
    cuts = [(0, width - 256), (width - 256, width)] if width % 256 == 0 and width > 256 else [(0, width)]
    hbm_spec = pl.BlockSpec(memory_space=pltpu.HBM)
    vmem_spec = pl.BlockSpec(memory_space=pltpu.VMEM)
    limit = 67043328 - 65536 - b * (-(-seq // 8) * 8) * width * 2
    exchange = pltpu.VMEM((n, pad, width), BF16)
    small = pltpu.VMEM((n, 1, width), F32)
    sems = pltpu.SemaphoreType.DMA((2,))
    sems_cut = pltpu.SemaphoreType.DMA((2, 2))
    ig, rg = pl.pallas_call(
        functools.partial(body, n, b, pad, chunk, tile, cuts),
        out_shape=(
            pltpu.VMEM((b, seq, width), BF16),
            pltpu.VMEM((1, width), F32),
        ),
        in_specs=[hbm_spec] * 9,
        out_specs=(vmem_spec, vmem_spec),
        scratch_shapes=[
            pltpu.VMEM(tokens.shape, BF16),
            pltpu.VMEM((b, n, seq), F32),
            pltpu.VMEM(slot_out.shape, BF16),
            pltpu.VMEM(slot_in.shape, BF16),
            pltpu.VMEM(out_grad.shape, BF16),
            pltpu.VMEM(router.shape, BF16),
            pltpu.VMEM(w_in.shape, BF16),
            pltpu.VMEM(bias_in.shape, F32),
            pltpu.VMEM(w_out.shape, BF16),
            pltpu.VMEM((b, n, seq), F32),
            pltpu.VMEM((b, n, seq), F32),
            pltpu.VMEM((b, n, seq), BF16),
            pltpu.VMEM((tall, b * span), BF16),
            pltpu.VMEM((b, n, seq), BF16),
            pltpu.VMEM((tall, b * span), F32),
            pltpu.VMEM((tall, b * span), F32),
            pltpu.VMEM((padded, hidden), F32),
            pltpu.VMEM((width // 128, padded, 128), F32),
            pltpu.VMEM((tall, width), BF16),
            pltpu.VMEM((n * b, width), BF16),
            pltpu.VMEM((padded, width), BF16),
            pltpu.VMEM((n, width), F32),
            pltpu.VMEM((padded, hidden), F32),
            pltpu.VMEM((b, n, seq), F32),
            exchange, exchange, exchange, exchange, exchange, exchange, small, small,
            pltpu.VMEM((width, b * span), BF16),
            pltpu.VMEM((padded, hidden), BF16),
            pltpu.VMEM((hidden, width), BF16),
            pltpu.VMEM((width, hidden), BF16),
            pltpu.SemaphoreType.DMA((9,)),
            pltpu.SemaphoreType.DMA((b,)),
            sems_cut, sems, pltpu.SemaphoreType.DMA((len(cuts), 3)), sems,
        ],
        compiler_params=pltpu.CompilerParams(
            collective_id=0, has_side_effects=True, vmem_limit_bytes=limit
        ),
        name="moe_input_grad",
    )(tokens, jnp.swapaxes(logits, 1, 2), slot_out, slot_in, out_grad, router, w_in, bias_in, w_out)
    return pl.pallas_call(
        write_out,
        out_shape=(jax.ShapeDtypeStruct(ig.shape, BF16), jax.ShapeDtypeStruct(rg.shape, F32)),
        in_specs=[vmem_spec, vmem_spec],
        out_specs=(hbm_spec, hbm_spec),
        scratch_shapes=[pltpu.SemaphoreType.DMA((b + 1,))],
        compiler_params=pltpu.CompilerParams(vmem_limit_bytes=1 << 20),
        name="write_out",
    )(
        pltpu.with_memory_space_constraint(ig, pltpu.VMEM),
        pltpu.with_memory_space_constraint(rg, pltpu.VMEM),
    )


def solution(mesh):
    placed = (
        P(("grp", "exp"), None, None),
        P(("grp", "exp"), None, None),
        P(("grp", "exp"), None, None),
        P(("grp", "exp"), None, None),
        P(("grp", "exp"), None, None),
        P(),
        P("exp", None, None),
        P("exp", None),
        P("exp", None, None),
    )
    return jax.shard_map(
        on_device,
        mesh=mesh,
        in_specs=placed,
        out_specs=(P(("grp", "exp"), None, None), P(("grp", "exp"), None)),
        check_vma=False,
    )
```

```python
import functools

import jax
import jax.numpy as jnp
from jax import lax
from jax.experimental import pallas as pl
from jax.experimental.pallas import tpu as pltpu
from jax.sharding import PartitionSpec as P

gelu_root = 0.7978845608028654
gelu_cubic = 0.044715
MESH = pl.DeviceIdType.MESH
F32 = jnp.float32
BF16 = jnp.bfloat16


def gelu_slope(values):
    square = values * values
    inner_arg = gelu_root * (values + gelu_cubic * square * values)
    tanh_val = jnp.tanh(inner_arg)
    return 0.5 * (1.0 + tanh_val) + 0.5 * values * (1.0 - tanh_val * tanh_val) * gelu_root * (
        1.0 + 3.0 * gelu_cubic * square
    )


def dot(a, b):
    return lax.dot_general(a, b, (((1,), (0,)), ((), ())), preferred_element_type=F32)


def dot_nt(a, b):
    return lax.dot_general(a, b, (((1,), (1,)), ((), ())), preferred_element_type=F32)


def dot_tn(a, b):
    return lax.dot_general(a, b, (((0,), (0,)), ((), ())), preferred_element_type=F32)


def ones_where(rows, cols, wanted):
    r = lax.broadcasted_iota(jnp.int32, (rows, cols), 0)
    c = lax.broadcasted_iota(jnp.int32, (rows, cols), 1)
    return jnp.where(wanted(r, c), 1.0, 0.0).astype(BF16)


def body(
    n, b, pad, chunk, tile, cuts,
    tok_hbm, log_hbm, so_hbm, si_hbm, og_hbm, rt_hbm, wi_hbm, bi_hbm, wo_hbm,
    ig_ref, rg_ref,
    tok, logv, so, si, og, rt, wi, bi, wo,
    comb, disp, combl, displ_a, displ_b, spread_disp, spread_dg, slope, sg, sig_a, sig_b, sip, rsum, part, dgs,
    send_s, recv_s, send_a, recv_a, send_b, recv_b, send_r, recv_r, tok_t, pre, wi_t, wo_t,
    load_sem, og_sem, sem_a, sem_s, sem_b, sem_r,
):
    me = lax.axis_index("exp")
    width = tok.shape[2]
    hidden = wi.shape[2]
    rows = n * b
    padded = n * pad
    lanes = 128
    seq = logv.shape[2]
    span = tok_t.shape[1] // b
    early = n // 4
    tall = early * pad

    barrier = pltpu.get_barrier_semaphore()

    def greet(d, _):
        peer = lax.rem(me + d, n)
        pl.semaphore_signal(barrier, inc=1, device_id={"exp": peer}, device_id_type=MESH)
        return 0

    def greet_all():
        lax.fori_loop(1, n, greet, 0, unroll=True)

    loads = {}
    pairs = [
        ("log", log_hbm, logv), ("og", og_hbm, og), ("si", si_hbm, si),
        ("wi", wi_hbm, wi), ("bi", bi_hbm, bi), ("wo", wo_hbm, wo), ("so", so_hbm, so), ("tok", tok_hbm, tok),
        ("rt", rt_hbm, rt),
    ]
    for at, (name, src, dst) in enumerate(pairs):
        loads[name] = pltpu.make_async_copy(src, dst, load_sem.at[at])
        if name == "og":
            for i in range(b):
                loads["og", i] = pltpu.make_async_copy(src.at[i], dst.at[i], og_sem.at[i])
                loads["og", i].start()
            continue
        if at == 2:
            greet_all()
        if name not in ("wo", "tok", "so", "rt"):
            loads[name].start()
    if span != seq:
        for i in range(b):
            tok_t[:, i * span + seq // lanes * lanes:(i + 1) * span] = jnp.zeros(
                (width, span - seq // lanes * lanes), BF16
            )

    def view(ref, at, cut):
        rows_sent = min(b, ref.shape[1])
        return ref.at[at, :rows_sent, cut[0]:cut[1]]

    g = 4 if n % 4 == 0 else 1
    block = me // g

    def peer_at(k):
        kb, w = k // g, k % g
        if k >= n - g:
            return me ^ (g - 1 - w)
        last = n // g - 1 - kb
        there = jnp.where(last + 1 > block, last + 1, last) if kb else 0
        there = jnp.where(block == 0, last, there)
        return there * g + ((me % g) ^ (g - 1 - w))

    def send_all(src, dst, sems, cut, first=0, last=n - 1):
        for k in range(first, last):
            peer = peer_at(k)
            pltpu.make_async_remote_copy(
                src_ref=view(src, peer, cut), dst_ref=view(dst, me, cut), send_sem=sems.at[0],
                recv_sem=sems.at[1], device_id={"exp": peer}, device_id_type=MESH,
            ).start()
        if last == n - 1:
            dst[me, :, cut[0]:cut[1]] = src[me, :, cut[0]:cut[1]]

    def everything(src, dst, sems, cut):
        return pltpu.make_async_remote_copy(
            src_ref=view(src, slice(0, n - 1), cut), dst_ref=view(dst, slice(0, n - 1), cut), send_sem=sems.at[0],
            recv_sem=sems.at[1], device_id={"exp": lax.rem(me + 1, n)}, device_id_type=MESH,
        )

    def wait_all(src, dst, sems, cut):
        everything(src, dst, sems, cut).wait_recv()

    def drain(src, dst, sems, cut):
        everything(src, dst, sems, cut).wait_send()

    whole = (0, width)
    spread = ones_where(padded, rows, lambda r, c: (r % pad < b) & (c == (r // pad) * b + r % pad))
    to_images = ones_where(rows, padded, lambda r, c: c == (r % n) * pad + r // n)

    def grouped(x):
        return x.reshape(n, pad, x.shape[1]).astype(BF16)

    def flat(x):
        wide = x.astype(F32)
        if pad != b:
            wide = jnp.where(lax.broadcasted_iota(jnp.int32, (1, pad, 1), 1) < b, wide, 0.0)
        return wide.reshape(x.shape[0] * pad, x.shape[2]).astype(BF16)

    def of_image(i):
        return slice(i * n, (i + 1) * n)

    loads["log"].wait()
    loads["wo"].start()
    loads["tok"].start()
    loads["so"].start()
    loads["rt"].start()
    for i in range(b):
        lt = logv[i]
        e = jnp.exp(lt - jnp.max(lt, axis=0, keepdims=True))
        comb[i] = e / jnp.sum(e, axis=0, keepdims=True)
    for i in range(b):
        loads["og", i].wait()
    for i in range(b):
        row = dot(comb[i].astype(BF16), og[i])
        for c in range(width // lanes):
            sg[c, pl.ds(i, n, stride=pad), :] = row[:, c * lanes:(c + 1) * lanes]
    for c in range(width // lanes):
        send_a[:, :, c * lanes:(c + 1) * lanes] = grouped(sg[c])
    def prepare():
        loads["si"].wait()
        sip[...] = dot(spread, si[0]).astype(BF16)
        loads["wi"].wait()
        loads["bi"].wait()
        for k in range(0, hidden, tile):
            hp = dot(sip[...], wi[0, :, k:k + tile]) + bi[:, k:k + tile]
            slope[:, k:k + tile] = gelu_slope(hp)
            wi_t[k:k + tile, :] = wi[0, :, k:k + tile].T

    pl.when(me < n // 8)(prepare)
    pl.semaphore_wait(barrier, n - 1)
    for q, cut in enumerate(cuts):
        send_all(send_a, recv_a, sem_a.at[q], cut, 0, n // 4)
    for q, cut in enumerate(cuts):
        send_all(send_a, recv_a, sem_a.at[q], cut, n // 4)

    pl.when(me >= n // 8)(prepare)

    for i in range(b):
        lt = logv[i]
        e = jnp.exp(lt - jnp.max(lt, axis=1, keepdims=True))
        disp[i] = e / jnp.sum(e, axis=1, keepdims=True)
    def send_slots():
        loads["so"].wait()
        send_s[...] = grouped(dot(spread, so[0]))
        send_all(send_s, recv_s, sem_s, whole)

    pl.when(me >= n // 8)(send_slots)
    loads["wo"].wait()
    for k in range(0, hidden, chunk):
        wo_t[:, k:k + chunk] = wo[0, k:k + chunk, :].T

    def turn_tokens():
        loads["tok"].wait()
        loads["rt"].wait()
        for i in range(b):
            tok_t[:, i * span:i * span + seq] = tok[i].T
        spread_disp[...] = jnp.zeros_like(spread_disp)
        for i in range(b):
            here = lax.broadcasted_iota(jnp.int32, (pad, seq), 0) == i
            for j in range(early):
                value = jnp.where(here, disp[i, j:j + 1, :], 0.0)
                spread_disp[j * pad:(j + 1) * pad, i * span:i * span + seq] = value

    pl.when(me < n // 8)(turn_tokens)
    pl.when(me < n // 8)(send_slots)
    for q, (lo, hi) in enumerate(cuts):
        wait_all(send_a, recv_a, sem_a.at[q], (lo, hi))
        got = flat(recv_a[:, :, lo:hi])
        for k in range(0, hidden, chunk):
            hg = dot(got, wo_t[lo:hi, k:k + chunk])
            if q > 0:
                hg = hg + part[:, k:k + chunk]
            if q < len(cuts) - 1:
                part[:, k:k + chunk] = hg
            else:
                pre[:, k:k + chunk] = (hg * slope[:, k:k + chunk]).astype(BF16)
    mine = jnp.minimum(me // early, 1)

    def send_rows(q, ks):
        lo, hi = cuts[q]
        for k in ks:
            peer = peer_at(k)
            pltpu.make_async_remote_copy(
                src_ref=send_b.at[peer, :b, lo:hi], dst_ref=recv_b.at[me, :b, lo:hi], send_sem=sem_b.at[q, 0],
                recv_sem=sem_b.at[q, 1 + mine], device_id={"exp": peer}, device_id_type=MESH,
            ).start()

    def rows_between(q, own):
        lo, hi = cuts[q]
        return pltpu.make_async_remote_copy(
            src_ref=send_b.at[own, :b, lo:hi], dst_ref=recv_b.at[own, :b, lo:hi], send_sem=sem_b.at[q, 0],
            recv_sem=sem_b.at[q, 1 + (own.start > 0)], device_id={"exp": lax.rem(me + 1, n)}, device_id_type=MESH,
        )

    for q, (lo, hi) in enumerate(cuts):
        @pl.when(me >= 0)
        def _():
            send_b[:, :, lo:hi] = grouped(dot(pre[...], wi_t[:, lo:hi]))
            send_rows(q, range(n // 4))
            pltpu.make_async_copy(
                send_b.at[me, :b, lo:hi], recv_b.at[me, :b, lo:hi], sem_b.at[q, 1 + mine]
            ).start()

    for k in range(n // 4, n - 1):
        for q in range(len(cuts)):
            send_rows(q, [k])

    pl.when(me >= n // 8)(turn_tokens)
    wait_all(send_s, recv_s, sem_s, whole)
    outs = dot(to_images, flat(recv_s[...])).astype(BF16)
    for i in range(b):
        dgs[i] = dot_nt(outs[of_image(i), :], og[i])
    for i in range(b):
        c, cg = comb[i], dgs[i]
        combl[i] = (c * (cg - jnp.sum(c * cg, axis=0, keepdims=True))).astype(BF16)

    def send_router(lo, hi):
        for j in range(lo, hi):
            @pl.when(me != j)
            def _():
                pltpu.make_async_remote_copy(
                    src_ref=send_r.at[j], dst_ref=recv_r.at[me], send_sem=sem_r.at[0],
                    recv_sem=sem_r.at[1], device_id={"exp": j}, device_id_type=MESH,
                ).start()

    for q, (lo, hi) in enumerate(cuts):
        rows_between(q, slice(0, early)).wait_recv()
        got = flat(recv_b[:early, :, lo:hi])
        sig_a[:, lo:hi] = got
        dg = dot(got, tok_t[lo:hi, :])
        if q > 0:
            dg = dg + spread_dg[...]
        if q < len(cuts) - 1:
            spread_dg[...] = dg
    d = spread_disp[...]
    part_sum = d * dg
    dl = (part_sum - d * jnp.sum(part_sum, axis=1, keepdims=True)).astype(BF16)
    displ_a[...] = dl
    racc = jnp.zeros((n + tall, width), F32)
    for i in range(b):
        terms = jnp.concatenate([combl[i], dl[:, i * span:i * span + seq]], axis=0)
        racc = racc + dot(terms, tok[i])
    rsum[...] = racc[:n]
    own = jnp.sum(racc[n:].reshape(early, pad, width), axis=1, keepdims=True)
    send_r[:early] = own + racc[:early].reshape(early, 1, width)
    send_router(0, early)

    to_image_rows = ones_where(
        rows, (n - early) * pad,
        lambda r, c: (c == (r % n - early) * pad + r // n) & (r % n >= early),
    )
    for q, (lo, hi) in enumerate(cuts):
        rows_between(q, slice(early, n)).wait_recv()
        sig_b[:, lo:hi] = dot(to_image_rows, flat(recv_b[early:, :, lo:hi])).astype(BF16)
        for i in range(b):
            dg = dot(sig_b[of_image(i), lo:hi], tok_t[lo:hi, i * span:i * span + seq])
            dgs[i] = dg if q == 0 else dgs[i] + dg
    racc = rsum[...]
    for i in range(b):
        d, dg = disp[i], dgs[i]
        dl = (d * (dg - jnp.sum(d * dg, axis=1, keepdims=True))).astype(BF16)
        displ_b[i] = dl
        racc = racc + dot(dl, tok[i])
    send_r[early:] = racc[early:].reshape(n - early, 1, width)
    send_router(early, n)
    recv_r[me] = send_r[me]

    spread_rt = dot(
        ones_where(tall, n, lambda r, c: c == r // pad), rt[...]
    ).astype(BF16)
    for i in range(b):
        at = slice(i * span, i * span + seq)
        left = jnp.concatenate(
            [spread_disp[:, at].astype(BF16), displ_a[:, at], disp[i].astype(BF16), combl[i], displ_b[i]], axis=0
        )
        right = jnp.concatenate(
            [sig_a[...], spread_rt, sig_b[of_image(i), :], rt[...], rt[...]], axis=0
        )
        ig_ref[i] = dot_tn(left, right).astype(BF16)

    drain(send_s, recv_s, sem_s, whole)
    for q, cut in enumerate(cuts):
        drain(send_a, recv_a, sem_a.at[q], cut)
    for q in range(len(cuts)):
        rows_between(q, slice(0, n - 1)).wait_send()
    wait_all(send_r, recv_r, sem_r, whole)
    rg_ref[...] = jnp.sum(recv_r[...], axis=0) / rows
    drain(send_r, recv_r, sem_r, whole)


def write_out(ig_ref, rg_ref, ig_hbm, rg_hbm, sems):
    copies = [pltpu.make_async_copy(rg_ref, rg_hbm, sems.at[0])]
    for i in range(ig_ref.shape[0]):
        copies.append(pltpu.make_async_copy(ig_ref.at[i], ig_hbm.at[i], sems.at[i + 1]))
    for copy in copies:
        copy.start()
    for copy in copies:
        copy.wait()


def on_device(tokens, logits, slot_out, slot_in, out_grad, router, w_in, bias_in, w_out):
    b, seq, width = tokens.shape
    n = lax.axis_size("exp")
    hidden = w_in.shape[2]
    pad = -(-b // 8) * 8
    padded = n * pad
    tall = n // 4 * pad
    span = -(-seq // 128) * 128
    chunk = 768 if hidden % 768 == 0 else hidden
    tile = 256 if hidden % 256 == 0 else hidden
    cuts = [(0, width - 256), (width - 256, width)] if width % 256 == 0 and width > 256 else [(0, width)]
    hbm_spec = pl.BlockSpec(memory_space=pltpu.HBM)
    vmem_spec = pl.BlockSpec(memory_space=pltpu.VMEM)
    limit = 67043328 - 65536 - b * (-(-seq // 8) * 8) * width * 2
    exchange = pltpu.VMEM((n, pad, width), BF16)
    small = pltpu.VMEM((n, 1, width), F32)
    sems = pltpu.SemaphoreType.DMA((2,))
    sems_cut = pltpu.SemaphoreType.DMA((2, 2))
    ig, rg = pl.pallas_call(
        functools.partial(body, n, b, pad, chunk, tile, cuts),
        out_shape=(
            pltpu.VMEM((b, seq, width), BF16),
            pltpu.VMEM((1, width), F32),
        ),
        in_specs=[hbm_spec] * 9,
        out_specs=(vmem_spec, vmem_spec),
        scratch_shapes=[
            pltpu.VMEM(tokens.shape, BF16),
            pltpu.VMEM((b, n, seq), F32),
            pltpu.VMEM(slot_out.shape, BF16),
            pltpu.VMEM(slot_in.shape, BF16),
            pltpu.VMEM(out_grad.shape, BF16),
            pltpu.VMEM(router.shape, BF16),
            pltpu.VMEM(w_in.shape, BF16),
            pltpu.VMEM(bias_in.shape, F32),
            pltpu.VMEM(w_out.shape, BF16),
            pltpu.VMEM((b, n, seq), F32),
            pltpu.VMEM((b, n, seq), F32),
            pltpu.VMEM((b, n, seq), BF16),
            pltpu.VMEM((tall, b * span), BF16),
            pltpu.VMEM((b, n, seq), BF16),
            pltpu.VMEM((tall, b * span), F32),
            pltpu.VMEM((tall, b * span), F32),
            pltpu.VMEM((padded, hidden), F32),
            pltpu.VMEM((width // 128, padded, 128), F32),
            pltpu.VMEM((tall, width), BF16),
            pltpu.VMEM((n * b, width), BF16),
            pltpu.VMEM((padded, width), BF16),
            pltpu.VMEM((n, width), F32),
            pltpu.VMEM((padded, hidden), F32),
            pltpu.VMEM((b, n, seq), F32),
            exchange, exchange, exchange, exchange, exchange, exchange, small, small,
            pltpu.VMEM((width, b * span), BF16),
            pltpu.VMEM((padded, hidden), BF16),
            pltpu.VMEM((hidden, width), BF16),
            pltpu.VMEM((width, hidden), BF16),
            pltpu.SemaphoreType.DMA((9,)),
            pltpu.SemaphoreType.DMA((b,)),
            sems_cut, sems, pltpu.SemaphoreType.DMA((len(cuts), 3)), sems,
        ],
        compiler_params=pltpu.CompilerParams(
            collective_id=0, has_side_effects=True, vmem_limit_bytes=limit
        ),
        name="moe_input_grad",
    )(tokens, jnp.swapaxes(logits, 1, 2), slot_out, slot_in, out_grad, router, w_in, bias_in, w_out)
    return pl.pallas_call(
        write_out,
        out_shape=(jax.ShapeDtypeStruct(ig.shape, BF16), jax.ShapeDtypeStruct(rg.shape, F32)),
        in_specs=[vmem_spec, vmem_spec],
        out_specs=(hbm_spec, hbm_spec),
        scratch_shapes=[pltpu.SemaphoreType.DMA((b + 1,))],
        compiler_params=pltpu.CompilerParams(vmem_limit_bytes=1 << 20),
        name="write_out",
    )(
        pltpu.with_memory_space_constraint(ig, pltpu.VMEM),
        pltpu.with_memory_space_constraint(rg, pltpu.VMEM),
    )


def solution(mesh):
    placed = (
        P(("grp", "exp"), None, None),
        P(("grp", "exp"), None, None),
        P(("grp", "exp"), None, None),
        P(("grp", "exp"), None, None),
        P(("grp", "exp"), None, None),
        P(),
        P("exp", None, None),
        P("exp", None),
        P("exp", None, None),
    )
    return jax.shard_map(
        on_device,
        mesh=mesh,
        in_specs=placed,
        out_specs=(P(("grp", "exp"), None, None), P(("grp", "exp"), None)),
        check_vma=False,
    )
```

```python
import functools

import jax
import jax.numpy as jnp
from jax import lax
from jax.experimental import pallas as pl
from jax.experimental.pallas import tpu as pltpu
from jax.sharding import PartitionSpec as P

gelu_root = 0.7978845608028654
gelu_cubic = 0.044715
MESH = pl.DeviceIdType.MESH
F32 = jnp.float32
BF16 = jnp.bfloat16


def gelu_slope(values):
    square = values * values
    inner_arg = gelu_root * (values + gelu_cubic * square * values)
    tanh_val = jnp.tanh(inner_arg)
    return 0.5 * (1.0 + tanh_val) + 0.5 * values * (1.0 - tanh_val * tanh_val) * gelu_root * (
        1.0 + 3.0 * gelu_cubic * square
    )


def dot(a, b):
    return lax.dot_general(a, b, (((1,), (0,)), ((), ())), preferred_element_type=F32)


def dot_nt(a, b):
    return lax.dot_general(a, b, (((1,), (1,)), ((), ())), preferred_element_type=F32)


def dot_tn(a, b):
    return lax.dot_general(a, b, (((0,), (0,)), ((), ())), preferred_element_type=F32)


def ones_where(rows, cols, wanted):
    r = lax.broadcasted_iota(jnp.int32, (rows, cols), 0)
    c = lax.broadcasted_iota(jnp.int32, (rows, cols), 1)
    return jnp.where(wanted(r, c), 1.0, 0.0).astype(BF16)


def body(
    n, b, pad, chunk, tile, cuts,
    tok_hbm, log_hbm, so_hbm, si_hbm, og_hbm, rt_hbm, wi_hbm, bi_hbm, wo_hbm,
    ig_ref, rg_ref,
    tok, logv, so, si, og, rt, wi, bi, wo,
    comb, disp, combl, displ_a, displ_b, spread_disp, spread_dg, slope, sg, sig_a, sig_b, sip, rsum, part, dgs,
    send_s, recv_s, send_a, recv_a, send_b, recv_b, send_r, recv_r, tok_t, pre, wi_t, wo_t,
    load_sem, og_sem, sem_a, sem_s, sem_b, sem_r,
):
    me = lax.axis_index("exp")
    width = tok.shape[2]
    hidden = wi.shape[2]
    rows = n * b
    padded = n * pad
    lanes = 128
    seq = logv.shape[2]
    span = tok_t.shape[1] // b
    early = n // 4
    tall = early * pad

    barrier = pltpu.get_barrier_semaphore()

    def greet(d, _):
        peer = lax.rem(me + d, n)
        pl.semaphore_signal(barrier, inc=1, device_id={"exp": peer}, device_id_type=MESH)
        return 0

    def greet_all():
        lax.fori_loop(1, n, greet, 0, unroll=True)

    loads = {}
    pairs = [
        ("log", log_hbm, logv), ("og", og_hbm, og), ("si", si_hbm, si),
        ("wi", wi_hbm, wi), ("bi", bi_hbm, bi), ("wo", wo_hbm, wo), ("so", so_hbm, so), ("tok", tok_hbm, tok),
        ("rt", rt_hbm, rt),
    ]
    for at, (name, src, dst) in enumerate(pairs):
        loads[name] = pltpu.make_async_copy(src, dst, load_sem.at[at])
        if name == "og":
            for i in range(b):
                loads["og", i] = pltpu.make_async_copy(src.at[i], dst.at[i], og_sem.at[i])
                loads["og", i].start()
            continue
        if at == 2:
            greet_all()
        if name not in ("wo", "tok", "so", "rt"):
            loads[name].start()
    if span != seq:
        for i in range(b):
            tok_t[:, i * span + seq // lanes * lanes:(i + 1) * span] = jnp.zeros(
                (width, span - seq // lanes * lanes), BF16
            )

    def view(ref, at, cut):
        rows_sent = min(b, ref.shape[1])
        return ref.at[at, :rows_sent, cut[0]:cut[1]]

    g = 4 if n % 4 == 0 else 1
    block = me // g

    def peer_at(k):
        kb, w = k // g, k % g
        if k >= n - g:
            return me ^ (g - 1 - w)
        last = n // g - 1 - kb
        there = jnp.where(last + 1 > block, last + 1, last) if kb else 0
        there = jnp.where(block == 0, last, there)
        return there * g + ((me % g) ^ (g - 1 - w))

    def peer_upward(k):
        kb, w = k // g, k % g
        if k >= n - g:
            return me ^ (g - 1 - w)
        last = n // g - 1 - kb
        there = jnp.where(last > block, last, last - 1)
        return jnp.where(block < n // g // 2, there * g + ((me % g) ^ (g - 1 - w)), peer_at(k))

    def send_all(src, dst, sems, cut, first=0, last=n - 1, order=peer_at):
        for k in range(first, last):
            peer = order(k)
            pltpu.make_async_remote_copy(
                src_ref=view(src, peer, cut), dst_ref=view(dst, me, cut), send_sem=sems.at[0],
                recv_sem=sems.at[1], device_id={"exp": peer}, device_id_type=MESH,
            ).start()
        if last == n - 1:
            dst[me, :, cut[0]:cut[1]] = src[me, :, cut[0]:cut[1]]

    def everything(src, dst, sems, cut):
        return pltpu.make_async_remote_copy(
            src_ref=view(src, slice(0, n - 1), cut), dst_ref=view(dst, slice(0, n - 1), cut), send_sem=sems.at[0],
            recv_sem=sems.at[1], device_id={"exp": lax.rem(me + 1, n)}, device_id_type=MESH,
        )

    def wait_all(src, dst, sems, cut):
        everything(src, dst, sems, cut).wait_recv()

    def drain(src, dst, sems, cut):
        everything(src, dst, sems, cut).wait_send()

    whole = (0, width)
    spread = ones_where(padded, rows, lambda r, c: (r % pad < b) & (c == (r // pad) * b + r % pad))
    to_images = ones_where(rows, padded, lambda r, c: c == (r % n) * pad + r // n)

    def grouped(x):
        return x.reshape(n, pad, x.shape[1]).astype(BF16)

    def flat(x):
        wide = x.astype(F32)
        if pad != b:
            wide = jnp.where(lax.broadcasted_iota(jnp.int32, (1, pad, 1), 1) < b, wide, 0.0)
        return wide.reshape(x.shape[0] * pad, x.shape[2]).astype(BF16)

    def of_image(i):
        return slice(i * n, (i + 1) * n)

    loads["log"].wait()
    loads["wo"].start()
    loads["tok"].start()
    loads["so"].start()
    loads["rt"].start()
    for i in range(b):
        lt = logv[i]
        e = jnp.exp(lt - jnp.max(lt, axis=0, keepdims=True))
        comb[i] = e / jnp.sum(e, axis=0, keepdims=True)
    for i in range(b):
        loads["og", i].wait()
    for i in range(b):
        row = dot(comb[i].astype(BF16), og[i])
        for c in range(width // lanes):
            sg[c, pl.ds(i, n, stride=pad), :] = row[:, c * lanes:(c + 1) * lanes]
    for c in range(width // lanes):
        send_a[:, :, c * lanes:(c + 1) * lanes] = grouped(sg[c])
    def prepare():
        loads["si"].wait()
        sip[...] = dot(spread, si[0]).astype(BF16)
        loads["wi"].wait()
        loads["bi"].wait()
        for k in range(0, hidden, tile):
            hp = dot(sip[...], wi[0, :, k:k + tile]) + bi[:, k:k + tile]
            slope[:, k:k + tile] = gelu_slope(hp)
            wi_t[k:k + tile, :] = wi[0, :, k:k + tile].T

    pl.when(me < n // 8)(prepare)
    pl.semaphore_wait(barrier, n - 1)
    for q, cut in enumerate(cuts):
        send_all(send_a, recv_a, sem_a.at[q], cut, 0, n // 4)
    for q, cut in enumerate(cuts):
        send_all(send_a, recv_a, sem_a.at[q], cut, n // 4)

    pl.when(me >= n // 8)(prepare)

    for i in range(b):
        lt = logv[i]
        e = jnp.exp(lt - jnp.max(lt, axis=1, keepdims=True))
        disp[i] = e / jnp.sum(e, axis=1, keepdims=True)
    def send_slots():
        loads["so"].wait()
        send_s[...] = grouped(dot(spread, so[0]))
        send_all(send_s, recv_s, sem_s, whole, order=peer_upward)

    pl.when(me >= n // 8)(send_slots)
    loads["wo"].wait()
    for k in range(0, hidden, chunk):
        wo_t[:, k:k + chunk] = wo[0, k:k + chunk, :].T

    def turn_tokens():
        loads["tok"].wait()
        loads["rt"].wait()
        for i in range(b):
            tok_t[:, i * span:i * span + seq] = tok[i].T
        spread_disp[...] = jnp.zeros_like(spread_disp)
        for i in range(b):
            here = lax.broadcasted_iota(jnp.int32, (pad, seq), 0) == i
            for j in range(early):
                value = jnp.where(here, disp[i, j:j + 1, :], 0.0)
                spread_disp[j * pad:(j + 1) * pad, i * span:i * span + seq] = value

    pl.when(me < n // 8)(turn_tokens)
    pl.when(me < n // 8)(send_slots)
    for q, (lo, hi) in enumerate(cuts):
        wait_all(send_a, recv_a, sem_a.at[q], (lo, hi))
        got = flat(recv_a[:, :, lo:hi])
        for k in range(0, hidden, chunk):
            hg = dot(got, wo_t[lo:hi, k:k + chunk])
            if q > 0:
                hg = hg + part[:, k:k + chunk]
            if q < len(cuts) - 1:
                part[:, k:k + chunk] = hg
            else:
                pre[:, k:k + chunk] = (hg * slope[:, k:k + chunk]).astype(BF16)
    mine = jnp.minimum(me // early, 1)

    def send_rows(q, ks):
        lo, hi = cuts[q]
        for k in ks:
            peer = peer_at(k)
            pltpu.make_async_remote_copy(
                src_ref=send_b.at[peer, :b, lo:hi], dst_ref=recv_b.at[me, :b, lo:hi], send_sem=sem_b.at[q, 0],
                recv_sem=sem_b.at[q, 1 + mine], device_id={"exp": peer}, device_id_type=MESH,
            ).start()

    def rows_between(q, own):
        lo, hi = cuts[q]
        return pltpu.make_async_remote_copy(
            src_ref=send_b.at[own, :b, lo:hi], dst_ref=recv_b.at[own, :b, lo:hi], send_sem=sem_b.at[q, 0],
            recv_sem=sem_b.at[q, 1 + (own.start > 0)], device_id={"exp": lax.rem(me + 1, n)}, device_id_type=MESH,
        )

    for q, (lo, hi) in enumerate(cuts):
        @pl.when(me >= 0)
        def _():
            send_b[:, :, lo:hi] = grouped(dot(pre[...], wi_t[:, lo:hi]))
            send_rows(q, range(n // 4))
            pltpu.make_async_copy(
                send_b.at[me, :b, lo:hi], recv_b.at[me, :b, lo:hi], sem_b.at[q, 1 + mine]
            ).start()

    for k in range(n // 4, n - 1):
        for q in range(len(cuts)):
            send_rows(q, [k])

    pl.when(me >= n // 8)(turn_tokens)
    wait_all(send_s, recv_s, sem_s, whole)
    outs = dot(to_images, flat(recv_s[...])).astype(BF16)
    for i in range(b):
        dgs[i] = dot_nt(outs[of_image(i), :], og[i])
    for i in range(b):
        c, cg = comb[i], dgs[i]
        combl[i] = (c * (cg - jnp.sum(c * cg, axis=0, keepdims=True))).astype(BF16)

    def send_router(lo, hi):
        for j in range(lo, hi):
            @pl.when(me != j)
            def _():
                pltpu.make_async_remote_copy(
                    src_ref=send_r.at[j], dst_ref=recv_r.at[me], send_sem=sem_r.at[0],
                    recv_sem=sem_r.at[1], device_id={"exp": j}, device_id_type=MESH,
                ).start()

    for q, (lo, hi) in enumerate(cuts):
        rows_between(q, slice(0, early)).wait_recv()
        got = flat(recv_b[:early, :, lo:hi])
        sig_a[:, lo:hi] = got
        dg = dot(got, tok_t[lo:hi, :])
        if q > 0:
            dg = dg + spread_dg[...]
        if q < len(cuts) - 1:
            spread_dg[...] = dg
    d = spread_disp[...]
    part_sum = d * dg
    dl = (part_sum - d * jnp.sum(part_sum, axis=1, keepdims=True)).astype(BF16)
    displ_a[...] = dl
    racc = jnp.zeros((n + tall, width), F32)
    for i in range(b):
        terms = jnp.concatenate([combl[i], dl[:, i * span:i * span + seq]], axis=0)
        racc = racc + dot(terms, tok[i])
    rsum[...] = racc[:n]
    own = jnp.sum(racc[n:].reshape(early, pad, width), axis=1, keepdims=True)
    send_r[:early] = own + racc[:early].reshape(early, 1, width)
    send_router(0, early)

    to_image_rows = ones_where(
        rows, (n - early) * pad,
        lambda r, c: (c == (r % n - early) * pad + r // n) & (r % n >= early),
    )
    for q, (lo, hi) in enumerate(cuts):
        rows_between(q, slice(early, n)).wait_recv()
        sig_b[:, lo:hi] = dot(to_image_rows, flat(recv_b[early:, :, lo:hi])).astype(BF16)
        for i in range(b):
            dg = dot(sig_b[of_image(i), lo:hi], tok_t[lo:hi, i * span:i * span + seq])
            dgs[i] = dg if q == 0 else dgs[i] + dg
    racc = rsum[...]
    for i in range(b):
        d, dg = disp[i], dgs[i]
        dl = (d * (dg - jnp.sum(d * dg, axis=1, keepdims=True))).astype(BF16)
        displ_b[i] = dl
        racc = racc + dot(dl, tok[i])
    send_r[early:] = racc[early:].reshape(n - early, 1, width)
    send_router(early, n)
    recv_r[me] = send_r[me]

    spread_rt = dot(
        ones_where(tall, n, lambda r, c: c == r // pad), rt[...]
    ).astype(BF16)
    for i in range(b):
        at = slice(i * span, i * span + seq)
        left = jnp.concatenate(
            [spread_disp[:, at].astype(BF16), displ_a[:, at], disp[i].astype(BF16), combl[i], displ_b[i]], axis=0
        )
        right = jnp.concatenate(
            [sig_a[...], spread_rt, sig_b[of_image(i), :], rt[...], rt[...]], axis=0
        )
        ig_ref[i] = dot_tn(left, right).astype(BF16)

    drain(send_s, recv_s, sem_s, whole)
    for q, cut in enumerate(cuts):
        drain(send_a, recv_a, sem_a.at[q], cut)
    for q in range(len(cuts)):
        rows_between(q, slice(0, n - 1)).wait_send()
    wait_all(send_r, recv_r, sem_r, whole)
    rg_ref[...] = jnp.sum(recv_r[...], axis=0) / rows
    drain(send_r, recv_r, sem_r, whole)


def write_out(ig_ref, rg_ref, ig_hbm, rg_hbm, sems):
    copies = [pltpu.make_async_copy(rg_ref, rg_hbm, sems.at[0])]
    for i in range(ig_ref.shape[0]):
        copies.append(pltpu.make_async_copy(ig_ref.at[i], ig_hbm.at[i], sems.at[i + 1]))
    for copy in copies:
        copy.start()
    for copy in copies:
        copy.wait()


def on_device(tokens, logits, slot_out, slot_in, out_grad, router, w_in, bias_in, w_out):
    b, seq, width = tokens.shape
    n = lax.axis_size("exp")
    hidden = w_in.shape[2]
    pad = -(-b // 8) * 8
    padded = n * pad
    tall = n // 4 * pad
    span = -(-seq // 128) * 128
    chunk = 768 if hidden % 768 == 0 else hidden
    tile = 256 if hidden % 256 == 0 else hidden
    cuts = [(0, width - 256), (width - 256, width)] if width % 256 == 0 and width > 256 else [(0, width)]
    hbm_spec = pl.BlockSpec(memory_space=pltpu.HBM)
    vmem_spec = pl.BlockSpec(memory_space=pltpu.VMEM)
    limit = 67043328 - 65536 - b * (-(-seq // 8) * 8) * width * 2
    exchange = pltpu.VMEM((n, pad, width), BF16)
    small = pltpu.VMEM((n, 1, width), F32)
    sems = pltpu.SemaphoreType.DMA((2,))
    sems_cut = pltpu.SemaphoreType.DMA((2, 2))
    ig, rg = pl.pallas_call(
        functools.partial(body, n, b, pad, chunk, tile, cuts),
        out_shape=(
            pltpu.VMEM((b, seq, width), BF16),
            pltpu.VMEM((1, width), F32),
        ),
        in_specs=[hbm_spec] * 9,
        out_specs=(vmem_spec, vmem_spec),
        scratch_shapes=[
            pltpu.VMEM(tokens.shape, BF16),
            pltpu.VMEM((b, n, seq), F32),
            pltpu.VMEM(slot_out.shape, BF16),
            pltpu.VMEM(slot_in.shape, BF16),
            pltpu.VMEM(out_grad.shape, BF16),
            pltpu.VMEM(router.shape, BF16),
            pltpu.VMEM(w_in.shape, BF16),
            pltpu.VMEM(bias_in.shape, F32),
            pltpu.VMEM(w_out.shape, BF16),
            pltpu.VMEM((b, n, seq), F32),
            pltpu.VMEM((b, n, seq), F32),
            pltpu.VMEM((b, n, seq), BF16),
            pltpu.VMEM((tall, b * span), BF16),
            pltpu.VMEM((b, n, seq), BF16),
            pltpu.VMEM((tall, b * span), F32),
            pltpu.VMEM((tall, b * span), F32),
            pltpu.VMEM((padded, hidden), F32),
            pltpu.VMEM((width // 128, padded, 128), F32),
            pltpu.VMEM((tall, width), BF16),
            pltpu.VMEM((n * b, width), BF16),
            pltpu.VMEM((padded, width), BF16),
            pltpu.VMEM((n, width), F32),
            pltpu.VMEM((padded, hidden), F32),
            pltpu.VMEM((b, n, seq), F32),
            exchange, exchange, exchange, exchange, exchange, exchange, small, small,
            pltpu.VMEM((width, b * span), BF16),
            pltpu.VMEM((padded, hidden), BF16),
            pltpu.VMEM((hidden, width), BF16),
            pltpu.VMEM((width, hidden), BF16),
            pltpu.SemaphoreType.DMA((9,)),
            pltpu.SemaphoreType.DMA((b,)),
            sems_cut, sems, pltpu.SemaphoreType.DMA((len(cuts), 3)), sems,
        ],
        compiler_params=pltpu.CompilerParams(
            collective_id=0, has_side_effects=True, vmem_limit_bytes=limit
        ),
        name="moe_input_grad",
    )(tokens, jnp.swapaxes(logits, 1, 2), slot_out, slot_in, out_grad, router, w_in, bias_in, w_out)
    return pl.pallas_call(
        write_out,
        out_shape=(jax.ShapeDtypeStruct(ig.shape, BF16), jax.ShapeDtypeStruct(rg.shape, F32)),
        in_specs=[vmem_spec, vmem_spec],
        out_specs=(hbm_spec, hbm_spec),
        scratch_shapes=[pltpu.SemaphoreType.DMA((b + 1,))],
        compiler_params=pltpu.CompilerParams(vmem_limit_bytes=1 << 20),
        name="write_out",
    )(
        pltpu.with_memory_space_constraint(ig, pltpu.VMEM),
        pltpu.with_memory_space_constraint(rg, pltpu.VMEM),
    )


def solution(mesh):
    placed = (
        P(("grp", "exp"), None, None),
        P(("grp", "exp"), None, None),
        P(("grp", "exp"), None, None),
        P(("grp", "exp"), None, None),
        P(("grp", "exp"), None, None),
        P(),
        P("exp", None, None),
        P("exp", None),
        P("exp", None, None),
    )
    return jax.shard_map(
        on_device,
        mesh=mesh,
        in_specs=placed,
        out_specs=(P(("grp", "exp"), None, None), P(("grp", "exp"), None)),
        check_vma=False,
    )
```
